128 devices in a mesh: ctx: 64 (over y_lo, x, z, core), head: 2 (over y_hi).
Axes of the slice: x: 4, y: 4 (y_hi: 2, y_lo: 2; y = y_hi * 2 + y_lo), z: 4, core: 2. Of those that a mesh axis runs over, the one named last changes fastest.
Arguments:
- queries: bfloat16 [16384, 32, 128], P('ctx', 'head'), may hold values from -300 to 300
- key_rows: bfloat16 [16384, 4, 128], P('ctx', 'head'), may hold values from -6 to 6
- value_vectors: bfloat16 [16384, 4, 128], P('ctx', 'head'), may hold values from -6 to 6
- doc_ids: int32 [16384], replicated, may hold values from 0 to 2, never falling along the last dimension, each value on 1 to 7936 neighbouring positions
Outputs:
- attended: bfloat16 [16384, 32, 128], P(('ctx', 'head'))
The draws below stay inside these ranges and needn't reach their ends.
Inputs may be any that keep to these rules, and one draw needn't show every extreme that they name: `doc_ids`: ids never fall along the pack and each prompt holds at most 7936 tokens.
All inputs are finite; a program needn't handle non-finite values.
Results may differ from the reference program's by a relative error of at most 0.008.
Values may be sent and summed in bfloat16 or wider, within the bound.
A program may use at most 64 MiB of HBM per device.

```python
import math
import jax
import jax.numpy as jnp
import numpy as np
from jax import lax

QUERY_HEADS = 32
KEY_VALUE_HEADS = 4
HEAD_SIZE = 128
TOKENS_PER_SHARD = 256
PROMPTS = 3
REACH = 31
PACKED_TOKENS = 16384
N_CTX = 64


def drawn_pair(key):
    key_sample = jax.random.fold_in(key, 11)
    query_draw = jax.random.fold_in(key, 23)
    key_entries = jnp.clip(jax.random.normal(key_sample, (PACKED_TOKENS, KEY_VALUE_HEADS, HEAD_SIZE), jnp.float32), -6.0, 6.0)
    query_vals = jnp.clip(jax.random.normal(query_draw, (PACKED_TOKENS, QUERY_HEADS, HEAD_SIZE), jnp.float32), -6.0, 6.0)
    return (query_vals, key_entries)


def draw_queries(key, part):
    return drawn_pair(key)[0].astype(jnp.bfloat16)


def draw_key_rows(key, part):
    return drawn_pair(key)[1].astype(jnp.bfloat16)


def steps_of(stream_key, dims, shards, smallest, largest):
    loudness = 1.0
    for dim, parts in shards:
        draws = jax.random.uniform(jax.random.fold_in(jax.random.fold_in(stream_key, 6), dim), (parts,), jnp.float32, smallest / len(shards), largest / len(shards))
        loudness = loudness * jnp.repeat(jnp.exp(draws), dims[dim] // parts).reshape((-1,) + (1,) * (len(dims) - 1 - dim))
    return loudness


def split_up(count, total, reach, lean):
    weights = [(1 << 20) // math.isqrt(rank ** lean) + 1 for rank in range(2, count + 1)]
    spare, given = total - reach - (count - 1), [1] * (count - 1)
    while spare > 0:
        candidates = [i for i in range(count - 1) if given[i] < reach]
        pool, left = sum([weights[i] for i in candidates]), spare
        for i in candidates:
            more = min(reach - given[i], max(1, left * weights[i] // pool), spare)
            given[i] = given[i] + more
            spare = spare - more
    return np.array([reach] + given)


def uneven(stream_key, count, total, limit, skew):
    if count == 2:
        one = jax.random.randint(stream_key, (), max(1, total - limit), min(limit, total - 1) + 1)
        return jnp.stack([one, total - one])
    lengths = jnp.asarray(split_up(count, total, limit, skew), jnp.int32)
    twos = (count - 1) // 2
    giver, taker = lengths[1:1 + 2 * twos:2], lengths[2:2 + 2 * twos:2]
    margin = jnp.minimum(giver - 1, limit - taker)
    shifted = jax.random.randint(jax.random.fold_in(stream_key, 1), (twos,), 0, 1 << 20) % (margin + 1)
    lengths = lengths.at[1:1 + 2 * twos:2].set(giver - shifted).at[2:2 + 2 * twos:2].set(taker + shifted)
    return lengths[jax.random.permutation(jax.random.fold_in(stream_key, 2), count)]


def noise(own_key, dims, scale, most, cuts=(), kind=jnp.bfloat16):
    loudness = steps_of(own_key, dims, cuts, -0.22, 0.18) if cuts else 1.0
    result = jax.random.normal(own_key, dims, jnp.float32) * scale * loudness
    return jnp.minimum(jnp.maximum(result, -most), most).astype(kind)


def setup_inputs(seed: int = 0) -> dict:
    key_of = jax.random.split(jax.random.key(seed), 5)
    return {
        "queries": draw_queries(jax.random.fold_in(key_of[4], 71), 0),
        "key_rows": draw_key_rows(jax.random.fold_in(key_of[4], 71), 0),
        "value_vectors": noise(key_of[2], (PACKED_TOKENS, KEY_VALUE_HEADS, HEAD_SIZE), 1.0, 6.0, ((0, 64), (1, 2))),
        "doc_ids": jnp.searchsorted(jnp.cumsum(uneven(key_of[3], PROMPTS, PACKED_TOKENS, REACH * TOKENS_PER_SHARD, 2)), jnp.arange(PACKED_TOKENS), side="right").astype(jnp.int32),
    }


def reference(queries, key_rows, value_vectors, doc_ids):
    head_group = QUERY_HEADS // KEY_VALUE_HEADS
    window = (REACH + 1) * TOKENS_PER_SHARD
    inv_root = HEAD_SIZE ** -0.5

    def query_block(block_num):
        query_offset = (block_num * TOKENS_PER_SHARD).astype(jnp.int32)
        k_start = jnp.maximum(query_offset - REACH * TOKENS_PER_SHARD, 0).astype(jnp.int32)
        query_portion = lax.dynamic_slice_in_dim(queries, query_offset, TOKENS_PER_SHARD, 0).reshape(TOKENS_PER_SHARD, KEY_VALUE_HEADS, head_group, HEAD_SIZE).astype(jnp.float32)
        k_part = lax.dynamic_slice_in_dim(key_rows, k_start, window, 0).astype(jnp.float32)
        v_part = lax.dynamic_slice_in_dim(value_vectors, k_start, window, 0).astype(jnp.float32)
        q_doc = lax.dynamic_slice_in_dim(doc_ids, query_offset, TOKENS_PER_SHARD, 0)
        k_doc = lax.dynamic_slice_in_dim(doc_ids, k_start, window, 0)
        q_pos = query_offset + jnp.arange(TOKENS_PER_SHARD, dtype=jnp.int32)
        k_pos = k_start + jnp.arange(window, dtype=jnp.int32)
        visible = (q_doc[:, None] == k_doc[None, :]) & (k_pos[None, :] <= q_pos[:, None])
        scores = jnp.einsum('tgrd,ugd->grtu', query_portion, k_part) * inv_root
        masked = jnp.where(visible, scores, -jnp.inf)
        row_max = jnp.max(masked, axis=-1, keepdims=True)
        weights = jnp.where(visible, jnp.exp(scores - row_max), 0.0)
        total = jnp.sum(weights, axis=-1, keepdims=True)
        rounded = lax.optimization_barrier(weights.astype(jnp.bfloat16)).astype(jnp.float32)
        summed = jnp.einsum('grtu,ugd->grtd', rounded, v_part) / total
        return summed.transpose(2, 0, 1, 3).reshape(TOKENS_PER_SHARD, QUERY_HEADS, HEAD_SIZE).astype(jnp.bfloat16)

    blocks = lax.map(query_block, jnp.arange(N_CTX, dtype=jnp.int32))
    return blocks.reshape(PACKED_TOKENS, QUERY_HEADS, HEAD_SIZE)
```

```python
import functools

import jax
import jax.numpy as jnp
from jax import lax
from jax.experimental import pallas as pl
from jax.experimental.pallas import tpu as pltpu
from jax.sharding import PartitionSpec as P

F32, BF16 = jnp.float32, jnp.bfloat16
MESH = pl.DeviceIdType.MESH
LOG2E = 1.4426950408889634
FAR = -1e30
T = 512
U = 2048
KB = 256
OWN0 = 72
UNITS = 73
NEAR = ((0, 3), (0, 1), (3, 0), (1, 0))
SECOND = ((0, 0), (2, 0), (0, 2), (1, 1))
THIRD = ((1, 3), (3, 1), (3, 3), (2, 1))
LAST = ((2, 3), (1, 2), (3, 2), (2, 2))
SLABS = ((0, NEAR), (1, NEAR), (0, SECOND), (0, THIRD), (0, LAST), (1, SECOND), (1, THIRD), (1, LAST))


def kernel(scale, q_ref, kv_ref, doc_ref, out_ref, buf, aug, qaug, s_ref, acc, mm, ll, obuf, sbuf,
           lsem, ssem, rsem, osend, orecv, fsem):
    i = lax.axis_index("ctx")
    h = lax.axis_index("head")
    k = lax.rem(i, 2)
    z = lax.rem(i // 2, 4)
    x = lax.rem(i // 8, 4)
    y = i // 32
    o = 1 - k
    up = lambda a: lax.rem(a + 1, 4)
    dn = lambda a: lax.rem(a + 3, 4)
    op = lambda a: lax.rem(a + 2, 4)

    def dev(yy, xx, zz, kk, hh=None):
        return {"ctx": ((yy * 4 + xx) * 4 + zz) * 2 + kk, "head": h if hh is None else hh}

    A = lambda zz, xx, kk: (zz * 4 + xx) * 2 + kk
    B = lambda xx, zz, kk: 32 + (xx * 4 + zz) * 2 + kk
    R = lambda zz, kk: 64 + zz * 2 + kk
    right_x, left_x = dev(y, up(x), z, k), dev(y, dn(x), z, k)
    right_z, left_z = dev(y, x, up(z), k), dev(y, x, dn(z), k)
    across, other = dev(1 - y, x, z, k), dev(y, x, z, o)
    mate = dev(y, x, z, k, 1 - h)

    sends = {}
    ending = [False]

    def copy(n, src, dst, to):
        return pltpu.make_async_remote_copy(
            src_ref=buf.at[src], dst_ref=buf.at[dst], send_sem=ssem.at[n], recv_sem=rsem.at[dst],
            device_id=to, device_id_type=MESH)

    def when(cond, f):
        if cond is None:
            f()
        else:
            pl.when(cond)(f)

    def send(name, src, dst, to, cond=None):
        n = sends.setdefault(name, len(sends))

        def go():
            c = copy(n, src, dst, to)
            c.wait_send() if ending[0] else c.start()

        when(cond, go)

    def arrived(u, cond=None):
        if not ending[0]:
            when(cond, lambda: copy(0, u, u, other).wait_recv())

    own = jnp.int32(OWN0)
    a_own, b_own = A(z, x, k), B(x, z, k)
    local = [(0, own, None), (1, b_own, None), (0, a_own, y == 0)] + [(1, R(n, k), y == 0) for n in range(4)]

    def local_copy(n):
        g, u, _ = local[n]
        return pltpu.make_async_copy(kv_ref.at[g], buf.at[u], lsem.at[n])

    for n in range(len(local)):
        when(local[n][2], lambda n=n: local_copy(n).start())
    barrier = pltpu.get_barrier_semaphore()
    for to in (right_x, left_x, right_z, left_z, across, other, mate):
        pl.semaphore_signal(barrier, inc=1, device_id=to, device_id_type=MESH)
    pl.semaphore_wait(barrier, 7)
    for n in range(len(local)):
        when(local[n][2], lambda n=n: local_copy(n).wait())

    def x_own(cond_r, cond_l):
        send("xr", jnp.where(x < 3, own, a_own), a_own, right_x, cond_r)
        send("xl", jnp.where(x > 0, a_own, own), a_own, left_x, cond_l)

    def z_own(cond_r, cond_l):
        send("zr", jnp.where(z < 3, own, a_own), a_own, right_z, cond_r)
        send("zl", jnp.where(z > 0, a_own, own), a_own, left_z, cond_l)

    def relay(name, even, place, at, to_r, to_l):
        src = jnp.where(even, place(dn(at)), place(up(at)))
        send(name + "r", src, src, to_r, even)
        send(name + "l", src, src, to_l, jnp.logical_not(even))

    def over(name, u, cond=None):
        send("o" + name, u, u, other, cond)

    x_even, z_even = lax.rem(x, 2) == 0, lax.rem(z, 2) == 0
    sign = {0: z_even, 1: jnp.logical_not(z_even), 2: z_even, 3: jnp.logical_not(z_even)}

    def row_on(n, zz):
        u = B(x, zz, k)
        send(f"y{n}", u, R(zz, k), across, y == 0)
        send(f"r{n}", jnp.where(x < 3, u, R(zz, k)), u, right_x, x < 3)
        send(f"l{n}", jnp.where(x > 0, R(zz, k), u), u, left_x, x == 0)

    def before_on(n, zz):
        arrived(R(zz, k), y == 1)
        u = B(x, zz, k)
        send(f"r{n}", jnp.where(x < 3, u, R(zz, k)), u, right_x, x == 3)
        send(f"l{n}", jnp.where(x > 0, R(zz, k), u), u, left_x, x > 0)
        if n == 0:
            over("p0", R(z, 1), k == 1)
        else:
            over(f"p{n}", R(zz, k), zz > z)

    zs = {0: z, 1: up(z), 2: op(z), 3: dn(z)}
    xs = {0: x, 1: up(x), 2: op(x), 3: dn(x)}

    def row_here(n):
        zz = zs[n]
        arrived(B(x, zz, k))
        row_on(n, zz)
        over(f"b{n}", B(x, zz, k), zz < z)

    def col_here(n):
        u = A(z, xs[n], k)
        arrived(u)
        send(f"zr{n}", u, u, right_z)
        send(f"zl{n}", u, u, left_z)
        over(f"a0{n}", u)

    def a_here(nx, nz):
        u = A(zs[nz], xs[nx], k)
        arrived(u)
        over(f"a{nz}{nx}", u)

    def a_relay(nx):
        a_here(nx, 1)
        a_here(nx, 3)
        relay(f"az{nx}", sign[nx], lambda zz: A(zz, xs[nx], k), z, right_z, left_z)

    def b_here(nx, nz):
        u = B(xs[nx], zs[nz], k)
        arrived(u)
        over(f"b{nx}{nz}", u)

    def b_relay(nz):
        b_here(1, nz)
        b_here(3, nz)
        relay(f"bx{nz}", x_even, lambda xx: B(xx, zs[nz], k), x, right_x, left_x)

    def handed(g, slab):
        for dx, dz in slab:
            xx, zz = xs[dx], zs[dz]
            if g == 0:
                arrived(A(zz, xx, o))
            elif dx:
                arrived(B(xx, zz, o))
            elif dz:
                arrived(jnp.where(zz < z, B(x, zz, o), R(zz, o)))
            else:
                arrived(jnp.where(k == 0, R(z, o), B(x, z, o)))

    def first():
        send("y", own, a_own, across, y == 0)
        send("bzr", b_own, b_own, right_z)
        send("bzl", b_own, b_own, left_z)
        x_own(x < 3, x == 0)
        z_own(z < 3, z == 0)
        row_on(0, z)
        send("own0", own, A(z, x, 0), other, k == 0)
        send("own1", b_own, B(x, z, 0), other, k == 0)

    first()

    docs = doc_ref[...]
    first1 = jnp.sum((docs < 1).astype(F32), keepdims=True).astype(jnp.int32)
    first2 = jnp.sum((docs < 2).astype(F32), keepdims=True).astype(jnp.int32)
    lane = lax.broadcasted_iota(jnp.int32, (1, 128), 1)
    none = jnp.int32(1 << 30)
    lo = jnp.where(lane == 0, 0, jnp.where(lane == 1, first1, jnp.where(lane == 2, first2, jnp.where(lane == 3, -none, none))))
    hi = jnp.where(lane == 0, first1, jnp.where(lane == 1, first2, jnp.where(lane == 2, none, jnp.where(lane == 3, 0, -none))))
    p = x * 4 + z
    me = i * 256

    def mark(u, _):
        c, kk = u // 2, lax.rem(u, 2)
        yy = jnp.where(c < p, y, y - 1)
        base = ((yy * 16 + c) * 2 + kk) * 256
        inner = jnp.where(kk == k, -100000, jnp.where(k == 0, ((y * 16 - 16 + c) * 2 + 1) * 256, (y * 16 + c) * 512))
        base = jnp.where(u == 32, me, jnp.where(c == p, inner, base))
        row = base + lax.broadcasted_iota(jnp.int32, (256, 128), 0)
        aug[u] = jnp.where((row >= lo) & (row < hi), 1.0, 0.0).astype(BF16)
        return 0

    lax.fori_loop(0, 33, mark, 0)
    pos = me + lax.broadcasted_iota(jnp.int32, (128, 256), 1)
    mine = (pos >= first1).astype(jnp.int32) + (pos >= first2).astype(jnp.int32)
    d = lax.broadcasted_iota(jnp.int32, (128, 256), 0)
    qaug[...] = jnp.where((d < 4) & ((d == 3) | (mine != d)), FAR, 0.0).astype(BF16)

    def query(jt):
        top = jnp.concatenate([q_ref[2 * jt], q_ref[2 * jt + 1]], axis=1)
        low = jnp.concatenate([qaug[...], qaug[...]], axis=1)
        return jnp.concatenate([top, low], axis=0)

    def keys(u, au):
        return jnp.concatenate([buf[u, 0:256, :], aug[au]], axis=1)

    def values(u):
        return jnp.concatenate([buf[u, 256:384, :], buf[u, 384:512, :]], axis=1)

    def eighths(a, f):
        return f(a.reshape(a.shape[0] // 8, 8, T), axis=0)

    def own_block(g):
        u = own if g == 0 else b_own

        def tile(j, _):
            jt = g * 4 + j
            s = jnp.dot(keys(u, 32), query(jt), preferred_element_type=F32)
            key = lax.broadcasted_iota(jnp.int32, (256, T), 0)
            tok = lax.rem(lax.broadcasted_iota(jnp.int32, (256, T), 1), 256)
            s = jnp.where(key <= tok, s, FAR)
            m = jnp.max(s, axis=0, keepdims=True)
            w = jnp.exp2((s - m) * scale)
            mm[jt] = m
            ll[jt] = eighths(w, jnp.sum)
            acc[jt] = jnp.dot(values(u), w.astype(BF16), preferred_element_type=F32)
            return 0

        lax.fori_loop(0, 4, tile, 0)

    def chips(g, slab):
        found = []
        for dx, dz in slab:
            xx, zz = xs[dx], zs[dz]
            if g == 0:
                c = zz * 4 + xx
            elif dx:
                c = 16 + xx * 4 + zz
            elif dz:
                c = jnp.where(zz < z, 16 + x * 4 + zz, 32 + zz)
            else:
                c = jnp.where(k == 0, 32 + z, 16 + x * 4 + z)
            found.append((c * 2, (xx * 4 + zz) * 2))
        return found

    def step(cur, jt, m_cur, nxt, jn):
        if nxt is not None:
            q = query(jn)
        if cur is not None:
            m_old = mm[jt]
            m_new = jnp.maximum(m_old, m_cur)
            alpha = jnp.exp2((m_old - m_new) * scale)
            mm[jt] = m_new
            out = acc[jt] * alpha
            total = ll[jt] * alpha
        best = None
        for b in range(U // KB):
            rows = slice(b * KB, (b + 1) * KB)
            if cur is not None:
                w = jnp.exp2((s_ref[rows] - m_new) * scale)
                total = total + eighths(w, jnp.sum)
                w = w.astype(BF16)
            if nxt is not None:
                u, au = nxt[b // 2]
                s = jnp.dot(keys(u + b % 2, au + b % 2), q, preferred_element_type=F32)
                high = eighths(s, jnp.max)
                best = high if best is None else jnp.maximum(best, high)
                s_ref[rows] = s
            if cur is not None:
                out = out + jnp.dot(values(cur[b // 2][0] + b % 2), w, preferred_element_type=F32)
        if cur is not None:
            acc[jt] = out
            ll[jt] = total
        return None if nxt is None else jnp.max(best, axis=0, keepdims=True)

    def finish(jt):
        total = jnp.sum(ll[jt], axis=0, keepdims=True)
        done = acc[jt] / total
        for n in range(2):
            head = done[:, n * 256:(n + 1) * 256].T.astype(BF16)
            keep = jnp.where(h == 0, head[:128], head[128:])
            give = jnp.where(h == 0, head[128:], head[:128])
            obuf[h * 16 + 2 * jt + n] = keep
            sbuf[2 * jt + n] = give

    def give(jt):
        return pltpu.make_async_remote_copy(
            src_ref=sbuf.at[pl.ds(2 * jt, 2)], dst_ref=obuf.at[pl.ds(h * 16 + 2 * jt, 2)],
            send_sem=osend.at[jt], recv_sem=orecv.at[jt], device_id=mate, device_id_type=MESH)

    def put(jt, whose):
        at = pl.ds(whose * 16 + 2 * jt, 2)
        return pltpu.make_async_copy(obuf.at[at], out_ref.at[at], fsem.at[jt + 8 * (0 if whose is h else 1)])

    def e1():
        arrived(a_own, y == 1)
        x_own(x == 3, x > 0)
        z_own(z == 3, z > 0)
        over("a00", A(z, x, 1), k == 1)

    def f1():
        row_here(1)
        row_here(3)
        relay("bz", z_even, lambda zz: B(x, zz, k), z, right_z, left_z)

    def e2():
        col_here(1)
        col_here(3)
        relay("ax", x_even, lambda xx: A(z, xx, k), x, right_x, left_x)

    def e3():
        a_relay(0)

    e1()
    own_block(0)
    f1()
    before_on(0, z)
    e2()
    own_block(1)
    e3()
    handed(*SLABS[0])

    events = {
        0: [(0, [(row_here, 2)]),
            (1, [(col_here, 2), (before_on, 1, zs[1]), (before_on, 3, zs[3])]),
            (2, [(a_here, 0, 2), (b_relay, 0)])],
        1: [(0, [(a_relay, 1)]), (1, [(before_on, 2, zs[2])]), (2, [(a_relay, 3), (b_relay, 1)])],
        2: [(0, [(a_relay, 2)]), (1, [(b_relay, 3)]), (2, [(a_here, 1, 2), (a_here, 3, 2), (b_here, 2, 0)])],
        3: [(0, [(b_relay, 2)]), (1, [(a_here, 2, 2)]), (2, [(b_here, 2, 1)])],
        4: [(0, [(b_here, 2, 3)]), (3, [(b_here, 2, 2)])],
    }

    def happen(event):
        for f, *args in event:
            f(*args)

    places = [chips(*s) for s in SLABS]
    m = step(None, None, None, places[0], SLABS[0][0] * 4)
    for n, (g, _) in enumerate(SLABS):
        cur = places[n]
        last = n == len(SLABS) - 1
        ends = n == 4 or last

        def one(j, m, n=n, g=g, cur=cur, last=last, ends=ends):
            for at, event in events.get(n, ()):
                pl.when(j == at)(lambda event=event: happen(event))
            if not last:
                pl.when(j == 3)(lambda: handed(*SLABS[n + 1]))
            jt = g * 4 + j
            if last:
                nxt, jn = cur, jt + 1
            else:
                nxt = [(jnp.where(j < 3, a, c), jnp.where(j < 3, b, d)) for (a, b), (c, d) in zip(cur, places[n + 1])]
                jn = jnp.where(j < 3, jt + 1, SLABS[n + 1][0] * 4)
            m = step(cur, jt, m, nxt, jn)
            if ends:
                @pl.when(j > 0)
                def _():
                    give(jt - 1).start()
                    put(jt - 1, h).start()
                finish(jt)
            return m

        m = lax.fori_loop(0, 3 if last else 4, one, m)
        if n == 4:
            give(3).start()
            put(3, h).start()
    give(6).start()
    put(6, h).start()
    step(places[7], 7, m, None, None)
    finish(7)
    give(7).start()
    put(7, h).start()
    theirs = 1 - h
    for jt in range(8):
        give(jt).wait_recv()
        put(jt, theirs).start()
    ending[0] = True
    for f in (first, e1, f1, lambda: before_on(0, z), e2, e3):
        f()
    for n in events:
        for _, event in events[n]:
            happen(event)
    for jt in range(8):
        give(jt).wait_send()
        put(jt, h).wait()
        put(jt, theirs).wait()


N_SENDS = 128


def body(queries, key_rows, value_vectors, doc_ids):
    tokens, heads, size = queries.shape
    groups = key_rows.shape[1]
    q = queries.transpose(1, 2, 0)
    kk = key_rows.transpose(1, 0, 2)
    vv = value_vectors.reshape(2, 128, groups, size).transpose(2, 0, 3, 1).reshape(groups, 256, 128)
    kv = jnp.concatenate([kk, vv], axis=1)
    scale = LOG2E * size ** -0.5
    vmem, anyspace = pl.BlockSpec(memory_space=pltpu.VMEM), pl.BlockSpec(memory_space=pl.ANY)
    out = pl.pallas_call(
        functools.partial(kernel, scale),
        out_shape=jax.ShapeDtypeStruct((2 * heads, 128, size), BF16),
        in_specs=[vmem, anyspace, vmem],
        out_specs=anyspace,
        scratch_shapes=[
            pltpu.VMEM((UNITS, 512, 128), BF16),
            pltpu.VMEM((33, 256, 128), BF16),
            pltpu.VMEM((128, 256), BF16),
            pltpu.VMEM((U, T), F32),
            pltpu.VMEM((8, 128, T), F32),
            pltpu.VMEM((8, 1, T), F32),
            pltpu.VMEM((8, 8, T), F32),
            pltpu.VMEM((2 * heads, 128, size), BF16),
            pltpu.VMEM((heads, 128, size), BF16),
            pltpu.SemaphoreType.DMA((7,)),
            pltpu.SemaphoreType.DMA((N_SENDS,)),
            pltpu.SemaphoreType.DMA((UNITS,)),
            pltpu.SemaphoreType.DMA((8,)),
            pltpu.SemaphoreType.DMA((8,)),
            pltpu.SemaphoreType.DMA((16,)),
        ],
        compiler_params=pltpu.CompilerParams(
            collective_id=0, has_side_effects=True, vmem_limit_bytes=60 * 1024 * 1024),
    )(q, kv, doc_ids.reshape(128, 128))
    return out.transpose(1, 0, 2)


def solution(mesh):
    placed = (P("ctx", "head", None), P("ctx", "head", None), P("ctx", "head", None), P())
    return jax.shard_map(
        body, mesh=mesh, in_specs=placed, out_specs=P(("ctx", "head"), None, None), check_vma=False
    )
```

```python
import functools

import jax
import jax.numpy as jnp
from jax import lax
from jax.experimental import pallas as pl
from jax.experimental.pallas import tpu as pltpu
from jax.sharding import PartitionSpec as P

F32, BF16 = jnp.float32, jnp.bfloat16
MESH = pl.DeviceIdType.MESH
LOG2E = 1.4426950408889634
FAR = -1e30
T = 512
U = 2048
KB = 256
OWN0 = 72
UNITS = 73
NEAR = ((0, 3), (0, 1), (3, 0), (1, 0))
SECOND = ((0, 0), (2, 0), (0, 2), (1, 1))
THIRD = ((1, 3), (3, 1), (3, 3), (2, 1))
LAST = ((2, 3), (1, 2), (3, 2), (2, 2))
TIMETABLE = {
    1: ("e1", "f1", "f1b"),
    2: ("p0",),
    3: ("e2b", "a0", "a0b", "e2"),
    5: ("row2",),
    6: ("p1", "b0", "p3"),
    7: ("b0b",),
    8: ("col2",),
    10: ("a1", "a3b", "a02", "a1b"),
    11: ("b3",),
    12: ("a2", "a3"),
    13: ("p2",),
    15: ("a12", "b1", "a2b"),
    17: ("b1b",),
    18: ("a32", "b2", "a22"),
    20: ("b2b", "b3b"),
    22: ("b23",),
    23: ("b20",),
    24: ("b21",),
    27: ("b22",),
}
SLABS = ((0, NEAR), (1, NEAR), (0, SECOND), (0, THIRD), (0, LAST), (1, SECOND), (1, THIRD), (1, LAST))


def kernel(scale, q_hbm, k_hbm, v_hbm, doc_ref, out_ref, q_raw, q_rows, q_ref, buf, aug, qaug, s_ref, acc, mm, ll, obuf, sbuf,
           lsem, qsem, ysem, ssem, rsem, osend, orecv, fsem):
    i = lax.axis_index("ctx")
    h = lax.axis_index("head")
    k = lax.rem(i, 2)
    z = lax.rem(i // 2, 4)
    x = lax.rem(i // 8, 4)
    y = i // 32
    o = 1 - k
    up = lambda a: lax.rem(a + 1, 4)
    dn = lambda a: lax.rem(a + 3, 4)
    op = lambda a: lax.rem(a + 2, 4)

    def dev(yy, xx, zz, kk, hh=None):
        return {"ctx": ((yy * 4 + xx) * 4 + zz) * 2 + kk, "head": h if hh is None else hh}

    A = lambda zz, xx, kk: (zz * 4 + xx) * 2 + kk
    B = lambda xx, zz, kk: 32 + (xx * 4 + zz) * 2 + kk
    R = lambda zz, kk: 64 + zz * 2 + kk
    right_x, left_x = dev(y, up(x), z, k), dev(y, dn(x), z, k)
    right_z, left_z = dev(y, x, up(z), k), dev(y, x, dn(z), k)
    across, other = dev(1 - y, x, z, k), dev(y, x, z, o)
    mate = dev(y, x, z, k, 1 - h)

    sends = {}
    ending = [False]

    def copy(n, src, dst, to, half=None, sem=None):
        part = () if half is None else (pl.ds(256 * half, 256),)
        return pltpu.make_async_remote_copy(
            src_ref=buf.at[(src,) + part], dst_ref=buf.at[(dst,) + part], send_sem=ssem.at[n],
            recv_sem=rsem.at[dst] if sem is None else sem, device_id=to, device_id_type=MESH)

    def when(cond, f):
        if cond is None:
            f()
        else:
            pl.when(cond)(f)

    def send(name, src, dst, to, cond=None, half=None, sem=None):
        n = sends.setdefault(name, len(sends))

        def go():
            c = copy(n, src, dst, to, half, sem)
            c.wait_send() if ending[0] else c.start()

        when(cond, go)

    def arrived(u, cond=None):
        if not ending[0]:
            when(cond, lambda: copy(0, u, u, other).wait_recv())

    own = jnp.int32(OWN0)
    a_own, b_own = A(z, x, k), B(x, z, k)
    local = [(0, own, None), (1, b_own, None), (0, a_own, y == 0)] + [(1, R(n, k), y == 0) for n in range(4)]

    class local_copy:
        def __init__(self, n):
            g, u, _ = local[n]
            self.both = [
                pltpu.make_async_copy(k_hbm.at[g], buf.at[u, 0:256], lsem.at[2 * n]),
                pltpu.make_async_copy(v_hbm.at[g], buf.at[u, 256:512], lsem.at[2 * n + 1])]

        def start(self):
            for c in self.both:
                c.start()

        def wait(self):
            for c in self.both:
                c.wait()

    for n in range(len(local)):
        when(local[n][2], lambda n=n: local_copy(n).start())
    load_q = pltpu.make_async_copy(q_hbm, q_raw, qsem)
    load_q.start()
    barrier = pltpu.get_barrier_semaphore()
    for to in (right_x, left_x, right_z, left_z, across, other, mate):
        pl.semaphore_signal(barrier, inc=1, device_id=to, device_id_type=MESH)
    pl.semaphore_wait(barrier, 7)
    for n in range(len(local)):
        when(local[n][2], lambda n=n: local_copy(n).wait())

    def relay(name, even, place, at, to_r, to_l):
        src = jnp.where(even, place(dn(at)), place(up(at)))
        send(name + "r", src, src, to_r, even)
        send(name + "l", src, src, to_l, jnp.logical_not(even))

    def over(name, u, cond=None):
        send("o" + name, u, u, other, cond)

    x_even, z_even = lax.rem(x, 2) == 0, lax.rem(z, 2) == 0
    sign = {0: z_even, 1: jnp.logical_not(z_even), 2: z_even, 3: jnp.logical_not(z_even)}

    def row_on(name, zz):
        u = B(x, zz, k)
        send(name + "y", u, R(zz, k), across, y == 0)
        send(name + "r", u, u, right_x, x < 3)
        send(name + "l", u, u, left_x, x == 0)

    def before_on(n, zz):
        arrived(R(zz, k), y == 1)
        u = B(x, zz, k)
        send(f"pr{n}", R(zz, k), u, right_x, x == 3)
        send(f"pl{n}", R(zz, k), u, left_x, x > 0)
        if n == 0:
            over("p0", R(z, 1), k == 1)
        else:
            over(f"p{n}", R(zz, k), zz > z)

    zs = {0: z, 1: up(z), 2: op(z), 3: dn(z)}
    xs = {0: x, 1: up(x), 2: op(x), 3: dn(x)}

    def nearer(even, at, first):
        return jnp.where(even == first, dn(at), up(at))

    def row_here(name, zz, first=False):
        arrived(B(x, zz, k))
        if first:
            relay("bz", z_even, lambda c: B(x, c, k), z, right_z, left_z)
        row_on(name, zz)
        over(name, B(x, zz, k), zz < z)

    def col_here(name, xx, first=False):
        u = A(z, xx, k)
        arrived(u)
        if first:
            relay("ax", x_even, lambda c: A(z, c, k), x, right_x, left_x)
        send(name + "zr", u, u, right_z)
        send(name + "zl", u, u, left_z)
        over(name, u)

    def a_here(n, zz, first=False):
        u = A(zz, xs[n], k)
        arrived(u)
        if first:
            relay(f"az{n}", sign[n], lambda c: A(c, xs[n], k), z, right_z, left_z)
        over(f"a{n}{'n' if first else 'f'}", u)

    def a_opposite(n):
        u = A(zs[2], xs[n], k)
        arrived(u)
        over(f"a{n}2", u)

    def b_here(n, xx, first=False):
        u = B(xx, zs[n], k)
        arrived(u)
        if first:
            relay(f"bx{n}", x_even, lambda c: B(c, zs[n], k), x, right_x, left_x)
        over(f"b{n}{'n' if first else 'f'}", u)

    def b_opposite(n):
        u = B(xs[2], zs[n], k)
        arrived(u)
        over(f"b2{n}", u)

    def previous():
        for half in range(2):
            if not ending[0]:
                when(y == 1, lambda: copy(0, a_own, a_own, other, half, ysem.at[half]).wait_recv())
            send(f"pxr{half}", a_own, a_own, right_x, x == 3, half)
            send(f"pxl{half}", a_own, a_own, left_x, x > 0, half)
            send(f"pzr{half}", a_own, a_own, right_z, z == 3, half)
            send(f"pzl{half}", a_own, a_own, left_z, z > 0, half)
        over("a00", A(z, x, 1), k == 1)

    happenings = {
        "e1": previous,
        "f1": lambda: row_here("f1", nearer(z_even, z, True), True),
        "f1b": lambda: row_here("f1b", nearer(z_even, z, False)),
        "row2": lambda: row_here("row2", zs[2]),
        "e2": lambda: col_here("e2", nearer(x_even, x, True), True),
        "e2b": lambda: col_here("e2b", nearer(x_even, x, False)),
        "col2": lambda: col_here("col2", xs[2]),
    }
    for n in range(4):
        happenings[f"p{n}"] = lambda n=n: before_on(n, zs[n])
        happenings[f"a{n}"] = lambda n=n: a_here(n, nearer(sign[n], z, True), True)
        happenings[f"a{n}b"] = lambda n=n: a_here(n, nearer(sign[n], z, False))
        happenings[f"a{n}2"] = lambda n=n: a_opposite(n)
        happenings[f"b{n}"] = lambda n=n: b_here(n, nearer(x_even, x, True), True)
        happenings[f"b{n}b"] = lambda n=n: b_here(n, nearer(x_even, x, False))
        happenings[f"b2{n}"] = lambda n=n: b_opposite(n)

    def handed(g, slab):
        for dx, dz in slab:
            xx, zz = xs[dx], zs[dz]
            if g == 0:
                arrived(A(zz, xx, o))
            elif dx:
                arrived(B(xx, zz, o))
            elif dz:
                arrived(jnp.where(zz < z, B(x, zz, o), R(zz, o)))
            else:
                arrived(jnp.where(k == 0, R(z, o), B(x, z, o)))

    def first():
        send("y0", own, a_own, across, y == 0, 0, ysem.at[0])
        send("y1", own, a_own, across, y == 0, 1, ysem.at[1])
        send("bzr", b_own, b_own, right_z)
        send("bzl", b_own, b_own, left_z)
        send("xr", own, a_own, right_x, x < 3)
        send("xl", own, a_own, left_x, x == 0)
        send("zr", own, a_own, right_z, z < 3)
        send("zl", own, a_own, left_z, z == 0)
        row_on("own", z)
        send("own0", own, A(z, x, 0), other, k == 0)
        send("own1", b_own, B(x, z, 0), other, k == 0)

    first()

    docs = doc_ref[...]
    first1 = jnp.sum((docs < 1).astype(F32), keepdims=True).astype(jnp.int32)
    first2 = jnp.sum((docs < 2).astype(F32), keepdims=True).astype(jnp.int32)
    lane = lax.broadcasted_iota(jnp.int32, (1, 128), 1)
    none = jnp.int32(1 << 30)
    lo = jnp.where(lane == 0, 0, jnp.where(lane == 1, first1, jnp.where(lane == 2, first2, jnp.where(lane == 3, -none, none))))
    hi = jnp.where(lane == 0, first1, jnp.where(lane == 1, first2, jnp.where(lane == 2, none, jnp.where(lane == 3, 0, -none))))
    p = x * 4 + z
    me = i * 256

    def mark(u, _):
        c, kk = u // 2, lax.rem(u, 2)
        yy = jnp.where(c < p, y, y - 1)
        base = ((yy * 16 + c) * 2 + kk) * 256
        inner = jnp.where(kk == k, -100000, jnp.where(k == 0, ((y * 16 - 16 + c) * 2 + 1) * 256, (y * 16 + c) * 512))
        base = jnp.where(u == 32, me, jnp.where(c == p, inner, base))
        row = base + lax.broadcasted_iota(jnp.int32, (256, 128), 0)
        aug[u] = jnp.where((row >= lo) & (row < hi), 1.0, 0.0).astype(BF16)
        return 0

    pos = me + lax.broadcasted_iota(jnp.int32, (128, 256), 1)
    mine = (pos >= first1).astype(jnp.int32) + (pos >= first2).astype(jnp.int32)
    d = lax.broadcasted_iota(jnp.int32, (128, 256), 0)
    qaug[...] = jnp.where((d < 4) & ((d == 3) | (mine != d)), FAR, 0.0).astype(BF16)

    def query(jt):
        top = jnp.concatenate([q_ref[2 * jt], q_ref[2 * jt + 1]], axis=1)
        low = jnp.concatenate([qaug[...], qaug[...]], axis=1)
        return jnp.concatenate([top, low], axis=0)

    def keys(u, au):
        return jnp.concatenate([buf[u, 0:256, :], aug[au]], axis=1)

    def values(u):
        return jnp.concatenate([buf[u, 256:384, :], buf[u, 384:512, :]], axis=1)

    def eighths(a, f):
        return f(a.reshape(a.shape[0] // 8, 8, T), axis=0)

    def own_block(g):
        u = own if g == 0 else b_own

        def tile(j, _):
            jt = g * 4 + j
            s = jnp.dot(keys(u, 32), query(jt), preferred_element_type=F32)
            key = lax.broadcasted_iota(jnp.int32, (256, T), 0)
            tok = lax.rem(lax.broadcasted_iota(jnp.int32, (256, T), 1), 256)
            s = jnp.where(key <= tok, s, FAR)
            m = jnp.max(s, axis=0, keepdims=True)
            w = jnp.exp2((s - m) * scale)
            mm[jt] = m
            ll[jt] = eighths(w, jnp.sum)
            acc[jt] = jnp.dot(values(u), w.astype(BF16), preferred_element_type=F32)
            return 0

        lax.fori_loop(0, 4, tile, 0)

    def chips(g, slab):
        found = []
        for dx, dz in slab:
            xx, zz = xs[dx], zs[dz]
            if g == 0:
                c = zz * 4 + xx
            elif dx:
                c = 16 + xx * 4 + zz
            elif dz:
                c = jnp.where(zz < z, 16 + x * 4 + zz, 32 + zz)
            else:
                c = jnp.where(k == 0, 32 + z, 16 + x * 4 + z)
            found.append((c * 2, (xx * 4 + zz) * 2))
        return found

    def step(cur, jt, m_cur, nxt, jn):
        if nxt is not None:
            q = query(jn)
        if cur is not None:
            m_old = mm[jt]
            m_new = jnp.maximum(m_old, m_cur)
            alpha = jnp.exp2((m_old - m_new) * scale)
            mm[jt] = m_new
            out = acc[jt] * alpha
            total = ll[jt] * alpha
        best = None
        for b in range(U // KB):
            rows = slice(b * KB, (b + 1) * KB)
            if cur is not None:
                w = jnp.exp2((s_ref[rows] - m_new) * scale)
                total = total + eighths(w, jnp.sum)
                w = w.astype(BF16)
            if nxt is not None:
                u, au = nxt[b // 2]
                s = jnp.dot(keys(u + b % 2, au + b % 2), q, preferred_element_type=F32)
                high = eighths(s, jnp.max)
                best = high if best is None else jnp.maximum(best, high)
                s_ref[rows] = s
            if cur is not None:
                out = out + jnp.dot(values(cur[b // 2][0] + b % 2), w, preferred_element_type=F32)
        if cur is not None:
            acc[jt] = out
            ll[jt] = total
        return None if nxt is None else jnp.max(best, axis=0, keepdims=True)

    def finish(jt):
        total = jnp.sum(ll[jt], axis=0, keepdims=True)
        done = acc[jt] / total
        for n in range(2):
            head = done[:, n * 256:(n + 1) * 256].T.astype(BF16)
            keep = jnp.where(h == 0, head[:128], head[128:])
            give = jnp.where(h == 0, head[128:], head[:128])
            obuf[h * 16 + 2 * jt + n] = keep
            sbuf[2 * jt + n] = give

    def give(jt):
        return pltpu.make_async_remote_copy(
            src_ref=sbuf.at[pl.ds(2 * jt, 2)], dst_ref=obuf.at[pl.ds(h * 16 + 2 * jt, 2)],
            send_sem=osend.at[jt], recv_sem=orecv.at[jt], device_id=mate, device_id_type=MESH)

    def put(jt, whose):
        at = pl.ds(whose * 16 + 2 * jt, 2)
        return pltpu.make_async_copy(obuf.at[at], out_ref.at[at], fsem.at[jt + 8 * (0 if whose is h else 1)])

    def happen(p):
        for name in TIMETABLE.get(p, ()):
            happenings[name]()

    happen(0)
    lax.fori_loop(0, 33, mark, 0)
    load_q.wait()
    r = lax.broadcasted_iota(jnp.int32, (256, 256), 0)
    c = lax.broadcasted_iota(jnp.int32, (256, 256), 1)
    order = jnp.where(c == lax.rem(r, 16) * 16 + r // 16, 1.0, 0.0).astype(BF16)

    def by_head(n, _):
        rows = q_raw[pl.ds(pl.multiple_of(n * 256, 256), 256), :]
        rows = jnp.dot(order, rows, preferred_element_type=F32).astype(BF16)
        for head in range(16):
            q_rows[head, pl.ds(pl.multiple_of(n * 16, 16), 16), :] = rows[head * 16:(head + 1) * 16]
        return 0

    def turn(n, _):
        q_ref[2 * n] = q_rows[2 * n].T
        q_ref[2 * n + 1] = q_rows[2 * n + 1].T
        return 0

    lax.fori_loop(0, 16, by_head, 0, unroll=8)
    lax.fori_loop(0, 8, turn, 0, unroll=4)
    happen(1)
    own_block(0)
    happen(2)
    own_block(1)
    happen(3)
    handed(*SLABS[0])
    places = [chips(*s) for s in SLABS]

    def out_of(jt):
        give(jt).start()
        put(jt, h).start()

    m = step(None, None, None, places[0], SLABS[0][0] * 4)
    for n in range(6):
        g, cur = SLABS[n][0], places[n]

        def one(j, m, n=n, g=g, cur=cur):
            for at in range(4):
                if 4 + 4 * n + at in TIMETABLE:
                    pl.when(j == at)(lambda at=at: happen(4 + 4 * n + at))
            pl.when(j == 3)(lambda: handed(*SLABS[n + 1]))
            jt = g * 4 + j
            nxt = [(jnp.where(j < 3, a, c), jnp.where(j < 3, b, d)) for (a, b), (c, d) in zip(cur, places[n + 1])]
            m = step(cur, jt, m, nxt, jnp.where(j < 3, jt + 1, SLABS[n + 1][0] * 4))
            if n == 4:
                pl.when(j > 0)(lambda: out_of(jt - 1))
                finish(jt)
            return m

        m = lax.fori_loop(0, 4, one, m)
        if n == 4:
            out_of(3)

    def two(j, m):
        @pl.when(j == 0)
        def _():
            happen(28)
            handed(*SLABS[7])
        jt = 4 + j
        m = step(places[6], jt, m, places[7], jt)
        pl.when(j > 0)(lambda: out_of(jt - 1))
        m = step(places[7], jt, m, places[6], jt + 1)
        finish(jt)
        return m

    m = lax.fori_loop(0, 3, two, m)
    m = step(places[6], 7, m, places[7], 7)
    out_of(6)
    step(places[7], 7, m, None, None)
    finish(7)
    out_of(7)
    theirs = 1 - h
    for jt in range(8):
        give(jt).wait_recv()
        put(jt, theirs).start()
    ending[0] = True
    first()
    for p in TIMETABLE:
        happen(p)
    for jt in range(8):
        give(jt).wait_send()
        put(jt, h).wait()
        put(jt, theirs).wait()


N_SENDS = 128


def body(queries, key_rows, value_vectors, doc_ids):
    tokens, heads, size = queries.shape
    groups = key_rows.shape[1]
    q = queries.reshape(tokens * heads, size)
    kk = key_rows.transpose(1, 0, 2)
    vv = value_vectors.reshape(2, 128, groups, size).transpose(2, 0, 3, 1).reshape(groups, 256, 128)
    scale = LOG2E * size ** -0.5
    vmem, anyspace = pl.BlockSpec(memory_space=pltpu.VMEM), pl.BlockSpec(memory_space=pl.ANY)
    out = pl.pallas_call(
        functools.partial(kernel, scale),
        out_shape=jax.ShapeDtypeStruct((2 * heads, 128, size), BF16),
        in_specs=[anyspace, anyspace, anyspace, vmem],
        out_specs=anyspace,
        scratch_shapes=[
            pltpu.VMEM((tokens * heads, size), BF16),
            pltpu.VMEM((heads, tokens, size), BF16),
            pltpu.VMEM((heads, size, tokens), BF16),
            pltpu.VMEM((UNITS, 512, 128), BF16),
            pltpu.VMEM((33, 256, 128), BF16),
            pltpu.VMEM((128, 256), BF16),
            pltpu.VMEM((U, T), F32),
            pltpu.VMEM((8, 128, T), F32),
            pltpu.VMEM((8, 1, T), F32),
            pltpu.VMEM((8, 8, T), F32),
            pltpu.VMEM((2 * heads, 128, size), BF16),
            pltpu.VMEM((heads, 128, size), BF16),
            pltpu.SemaphoreType.DMA((14,)),
            pltpu.SemaphoreType.DMA,
            pltpu.SemaphoreType.DMA((2,)),
            pltpu.SemaphoreType.DMA((N_SENDS,)),
            pltpu.SemaphoreType.DMA((UNITS,)),
            pltpu.SemaphoreType.DMA((8,)),
            pltpu.SemaphoreType.DMA((8,)),
            pltpu.SemaphoreType.DMA((16,)),
        ],
        compiler_params=pltpu.CompilerParams(
            collective_id=0, has_side_effects=True, vmem_limit_bytes=60 * 1024 * 1024),
    )(q, kk, vv, doc_ids.reshape(128, 128))
    return out.transpose(1, 0, 2)


def solution(mesh):
    placed = (P("ctx", "head", None), P("ctx", "head", None), P("ctx", "head", None), P())
    return jax.shard_map(
        body, mesh=mesh, in_specs=placed, out_specs=P(("ctx", "head"), None, None), check_vma=False
    )
```

```python
import functools

import jax
import jax.numpy as jnp
from jax import lax
from jax.experimental import pallas as pl
from jax.experimental.pallas import tpu as pltpu
from jax.sharding import PartitionSpec as P

F32, BF16 = jnp.float32, jnp.bfloat16
MESH = pl.DeviceIdType.MESH
LOG2E = 1.4426950408889634
FAR = -1e30
T = 512
U = 2048
KB = 256
OWN0 = 72
UNITS = 73
NEAR = ((0, 3), (0, 1), (3, 0), (1, 0))
SECOND = ((0, 0), (2, 0), (0, 2), (1, 1))
THIRD = ((1, 3), (3, 1), (3, 3), (2, 1))
LAST = ((2, 3), (1, 2), (3, 2), (2, 2))
TIMETABLE = {
    1: ("e1", "f1", "f1b"),
    2: ("p0",),
    3: ("e2b", "a0", "a0b", "e2"),
    4: ("row2", "p1", "b0", "p3"),
    5: ("b0b",),
    6: ("col2",),
    8: ("a1", "a3b", "a02", "a1b"),
    9: ("b3",),
    10: ("a2", "a3"),
    11: ("p2",),
    13: ("a12", "b1", "a2b"),
    15: ("b1b",),
    16: ("a32", "b2", "a22"),
    18: ("b2b", "b3b"),
    20: ("b23",),
    21: ("b20",),
    22: ("b21",),
    25: ("b22",),
}
SLABS = ((0, NEAR), (1, NEAR), (0, SECOND), (0, THIRD), (0, LAST), (1, SECOND), (1, THIRD), (1, LAST))


def kernel(scale, q_hbm, k_hbm, v_hbm, doc_ref, out_ref, q_raw, q_rows, q_ref, buf, aug, qaug, s_ref, acc, mm, ll, obuf, sbuf,
           lsem, qsem, ysem, ssem, rsem, osend, orecv, fsem):
    i = lax.axis_index("ctx")
    h = lax.axis_index("head")
    k = lax.rem(i, 2)
    z = lax.rem(i // 2, 4)
    x = lax.rem(i // 8, 4)
    y = i // 32
    o = 1 - k
    up = lambda a: lax.rem(a + 1, 4)
    dn = lambda a: lax.rem(a + 3, 4)
    op = lambda a: lax.rem(a + 2, 4)

    def dev(yy, xx, zz, kk, hh=None):
        return {"ctx": ((yy * 4 + xx) * 4 + zz) * 2 + kk, "head": h if hh is None else hh}

    A = lambda zz, xx, kk: (zz * 4 + xx) * 2 + kk
    B = lambda xx, zz, kk: 32 + (xx * 4 + zz) * 2 + kk
    R = lambda zz, kk: 64 + zz * 2 + kk
    right_x, left_x = dev(y, up(x), z, k), dev(y, dn(x), z, k)
    right_z, left_z = dev(y, x, up(z), k), dev(y, x, dn(z), k)
    across, other = dev(1 - y, x, z, k), dev(y, x, z, o)
    mate = dev(y, x, z, k, 1 - h)

    sends = {}
    ending = [False]

    def copy(n, src, dst, to, half=None, sem=None):
        part = () if half is None else (pl.ds(256 * half, 256),)
        return pltpu.make_async_remote_copy(
            src_ref=buf.at[(src,) + part], dst_ref=buf.at[(dst,) + part], send_sem=ssem.at[n],
            recv_sem=rsem.at[dst] if sem is None else sem, device_id=to, device_id_type=MESH)

    def when(cond, f):
        if cond is None:
            f()
        else:
            pl.when(cond)(f)

    def send(name, src, dst, to, cond=None, half=None, sem=None):
        n = sends.setdefault(name, len(sends))

        def go():
            c = copy(n, src, dst, to, half, sem)
            c.wait_send() if ending[0] else c.start()

        when(cond, go)

    def arrived(u, cond=None):
        if not ending[0]:
            when(cond, lambda: copy(0, u, u, other).wait_recv())

    own = jnp.int32(OWN0)
    a_own, b_own = A(z, x, k), B(x, z, k)
    local = [(0, own, None), (1, b_own, None), (0, a_own, y == 0)] + [(1, R(n, k), y == 0) for n in range(4)]

    class local_copy:
        def __init__(self, n):
            g, u, _ = local[n]
            self.both = [
                pltpu.make_async_copy(k_hbm.at[g], buf.at[u, 0:256], lsem.at[2 * n]),
                pltpu.make_async_copy(v_hbm.at[g], buf.at[u, 256:512], lsem.at[2 * n + 1])]

        def start(self):
            for c in self.both:
                c.start()

        def wait(self):
            for c in self.both:
                c.wait()

    for n in range(len(local)):
        when(local[n][2], lambda n=n: local_copy(n).start())
    load_q = pltpu.make_async_copy(q_hbm, q_raw, qsem)
    load_q.start()
    barrier = pltpu.get_barrier_semaphore()
    for to in (right_x, left_x, right_z, left_z, across, other, mate):
        pl.semaphore_signal(barrier, inc=1, device_id=to, device_id_type=MESH)
    pl.semaphore_wait(barrier, 7)
    for n in range(len(local)):
        when(local[n][2], lambda n=n: local_copy(n).wait())

    def relay(name, even, place, at, to_r, to_l):
        src = jnp.where(even, place(dn(at)), place(up(at)))
        send(name + "r", src, src, to_r, even)
        send(name + "l", src, src, to_l, jnp.logical_not(even))

    def over(name, u, cond=None):
        send("o" + name, u, u, other, cond)

    x_even, z_even = lax.rem(x, 2) == 0, lax.rem(z, 2) == 0
    sign = {0: z_even, 1: jnp.logical_not(z_even), 2: z_even, 3: jnp.logical_not(z_even)}

    def row_on(name, zz):
        u = B(x, zz, k)
        send(name + "y", u, R(zz, k), across, y == 0)
        send(name + "r", u, u, right_x, x < 3)
        send(name + "l", u, u, left_x, x == 0)

    def before_on(n, zz):
        arrived(R(zz, k), y == 1)
        u = B(x, zz, k)
        send(f"pr{n}", R(zz, k), u, right_x, x == 3)
        send(f"pl{n}", R(zz, k), u, left_x, x > 0)
        if n == 0:
            over("p0", R(z, 1), k == 1)
        else:
            over(f"p{n}", R(zz, k), zz > z)

    zs = {0: z, 1: up(z), 2: op(z), 3: dn(z)}
    xs = {0: x, 1: up(x), 2: op(x), 3: dn(x)}

    def nearer(even, at, first):
        return jnp.where(even == first, dn(at), up(at))

    def row_here(name, zz, first=False):
        arrived(B(x, zz, k))
        if first:
            relay("bz", z_even, lambda c: B(x, c, k), z, right_z, left_z)
        row_on(name, zz)
        over(name, B(x, zz, k), zz < z)

    def col_here(name, xx, first=False):
        u = A(z, xx, k)
        arrived(u)
        if first:
            relay("ax", x_even, lambda c: A(z, c, k), x, right_x, left_x)
        send(name + "zr", u, u, right_z)
        send(name + "zl", u, u, left_z)
        over(name, u)

    def a_here(n, zz, first=False):
        u = A(zz, xs[n], k)
        arrived(u)
        if first:
            relay(f"az{n}", sign[n], lambda c: A(c, xs[n], k), z, right_z, left_z)
        over(f"a{n}{'n' if first else 'f'}", u)

    def a_opposite(n):
        u = A(zs[2], xs[n], k)
        arrived(u)
        over(f"a{n}2", u)

    def b_here(n, xx, first=False):
        u = B(xx, zs[n], k)
        arrived(u)
        if first:
            relay(f"bx{n}", x_even, lambda c: B(c, zs[n], k), x, right_x, left_x)
        over(f"b{n}{'n' if first else 'f'}", u)

    def b_opposite(n):
        u = B(xs[2], zs[n], k)
        arrived(u)
        over(f"b2{n}", u)

    def previous():
        for half in range(2):
            if not ending[0]:
                when(y == 1, lambda: copy(0, a_own, a_own, other, half, ysem.at[half]).wait_recv())
            send(f"pxr{half}", a_own, a_own, right_x, x == 3, half)
            send(f"pxl{half}", a_own, a_own, left_x, x > 0, half)
            send(f"pzr{half}", a_own, a_own, right_z, z == 3, half)
            send(f"pzl{half}", a_own, a_own, left_z, z > 0, half)
        over("a00", A(z, x, 1), k == 1)

    happenings = {
        "e1": previous,
        "f1": lambda: row_here("f1", nearer(z_even, z, True), True),
        "f1b": lambda: row_here("f1b", nearer(z_even, z, False)),
        "row2": lambda: row_here("row2", zs[2]),
        "e2": lambda: col_here("e2", nearer(x_even, x, True), True),
        "e2b": lambda: col_here("e2b", nearer(x_even, x, False)),
        "col2": lambda: col_here("col2", xs[2]),
    }
    for n in range(4):
        happenings[f"p{n}"] = lambda n=n: before_on(n, zs[n])
        happenings[f"a{n}"] = lambda n=n: a_here(n, nearer(sign[n], z, True), True)
        happenings[f"a{n}b"] = lambda n=n: a_here(n, nearer(sign[n], z, False))
        happenings[f"a{n}2"] = lambda n=n: a_opposite(n)
        happenings[f"b{n}"] = lambda n=n: b_here(n, nearer(x_even, x, True), True)
        happenings[f"b{n}b"] = lambda n=n: b_here(n, nearer(x_even, x, False))
        happenings[f"b2{n}"] = lambda n=n: b_opposite(n)

    def handed(g, slab):
        for dx, dz in slab:
            xx, zz = xs[dx], zs[dz]
            if g == 0:
                arrived(A(zz, xx, o))
            elif dx:
                arrived(B(xx, zz, o))
            elif dz:
                arrived(jnp.where(zz < z, B(x, zz, o), R(zz, o)))
            else:
                arrived(jnp.where(k == 0, R(z, o), B(x, z, o)))

    def first():
        send("y0", own, a_own, across, y == 0, 0, ysem.at[0])
        send("y1", own, a_own, across, y == 0, 1, ysem.at[1])
        send("bzr", b_own, b_own, right_z)
        send("bzl", b_own, b_own, left_z)
        send("xr", own, a_own, right_x, x < 3)
        send("xl", own, a_own, left_x, x == 0)
        send("zr", own, a_own, right_z, z < 3)
        send("zl", own, a_own, left_z, z == 0)
        row_on("own", z)
        send("own0", own, A(z, x, 0), other, k == 0)
        send("own1", b_own, B(x, z, 0), other, k == 0)

    first()

    docs = doc_ref[...]
    first1 = jnp.sum((docs < 1).astype(F32), keepdims=True).astype(jnp.int32)
    first2 = jnp.sum((docs < 2).astype(F32), keepdims=True).astype(jnp.int32)
    lane = lax.broadcasted_iota(jnp.int32, (1, 128), 1)
    none = jnp.int32(1 << 30)
    lo = jnp.where(lane == 0, 0, jnp.where(lane == 1, first1, jnp.where(lane == 2, first2, jnp.where(lane == 3, -none, none))))
    hi = jnp.where(lane == 0, first1, jnp.where(lane == 1, first2, jnp.where(lane == 2, none, jnp.where(lane == 3, 0, -none))))
    p = x * 4 + z
    me = i * 256

    def mark(u, _):
        c, kk = u // 2, lax.rem(u, 2)
        yy = jnp.where(c < p, y, y - 1)
        base = ((yy * 16 + c) * 2 + kk) * 256
        inner = jnp.where(kk == k, -100000, jnp.where(k == 0, ((y * 16 - 16 + c) * 2 + 1) * 256, (y * 16 + c) * 512))
        base = jnp.where(u == 32, me, jnp.where(c == p, inner, base))
        row = base + lax.broadcasted_iota(jnp.int32, (256, 128), 0)
        aug[u] = jnp.where((row >= lo) & (row < hi), 1.0, 0.0).astype(BF16)
        return 0

    pos = me + lax.broadcasted_iota(jnp.int32, (128, 256), 1)
    mine = (pos >= first1).astype(jnp.int32) + (pos >= first2).astype(jnp.int32)
    d = lax.broadcasted_iota(jnp.int32, (128, 256), 0)
    qaug[...] = jnp.where((d < 4) & ((d == 3) | (mine != d)), FAR, 0.0).astype(BF16)

    def query(jt):
        top = jnp.concatenate([q_ref[2 * jt], q_ref[2 * jt + 1]], axis=1)
        low = jnp.concatenate([qaug[...], qaug[...]], axis=1)
        return jnp.concatenate([top, low], axis=0)

    def keys(u, au):
        return jnp.concatenate([buf[u, 0:256, :], aug[au]], axis=1)

    def values(u):
        return jnp.concatenate([buf[u, 256:384, :], buf[u, 384:512, :]], axis=1)

    def eighths(a, f):
        return f(a.reshape(a.shape[0] // 8, 8, T), axis=0)

    def own_block(g):
        u = own if g == 0 else b_own

        def tile(j, _):
            jt = g * 4 + j
            s = jnp.dot(keys(u, 32), query(jt), preferred_element_type=F32)
            key = lax.broadcasted_iota(jnp.int32, (256, T), 0)
            tok = lax.rem(lax.broadcasted_iota(jnp.int32, (256, T), 1), 256)
            s = jnp.where(key <= tok, s, FAR)
            m = jnp.max(s, axis=0, keepdims=True)
            w = jnp.exp2((s - m) * scale)
            mm[jt] = m
            ll[jt] = eighths(w, jnp.sum)
            acc[jt] = jnp.dot(values(u), w.astype(BF16), preferred_element_type=F32)
            return 0

        lax.fori_loop(0, 4, tile, 0)

    def chips(g, slab):
        found = []
        for dx, dz in slab:
            xx, zz = xs[dx], zs[dz]
            if g == 0:
                c = zz * 4 + xx
            elif dx:
                c = 16 + xx * 4 + zz
            elif dz:
                c = jnp.where(zz < z, 16 + x * 4 + zz, 32 + zz)
            else:
                c = jnp.where(k == 0, 32 + z, 16 + x * 4 + z)
            found.append((c * 2, (xx * 4 + zz) * 2))
        return found

    def step(cur, jt, m_cur, nxt, jn):
        if nxt is not None:
            q = query(jn)
        if cur is not None:
            m_old = mm[jt]
            m_new = jnp.maximum(m_old, m_cur)
            alpha = jnp.exp2((m_old - m_new) * scale)
            mm[jt] = m_new
            out = acc[jt] * alpha
            total = ll[jt] * alpha
        best = None
        for b in range(U // KB):
            rows = slice(b * KB, (b + 1) * KB)
            if cur is not None:
                w = jnp.exp2((s_ref[rows] - m_new) * scale)
                total = total + eighths(w, jnp.sum)
                w = w.astype(BF16)
            if nxt is not None:
                u, au = nxt[b // 2]
                s = jnp.dot(keys(u + b % 2, au + b % 2), q, preferred_element_type=F32)
                high = eighths(s, jnp.max)
                best = high if best is None else jnp.maximum(best, high)
                s_ref[rows] = s
            if cur is not None:
                out = out + jnp.dot(values(cur[b // 2][0] + b % 2), w, preferred_element_type=F32)
        if cur is not None:
            acc[jt] = out
            ll[jt] = total
        return None if nxt is None else jnp.max(best, axis=0, keepdims=True)

    def finish(jt):
        total = jnp.sum(ll[jt], axis=0, keepdims=True)
        done = acc[jt] / total
        for n in range(2):
            head = done[:, n * 256:(n + 1) * 256].T.astype(BF16)
            keep = jnp.where(h == 0, head[:128], head[128:])
            give = jnp.where(h == 0, head[128:], head[:128])
            obuf[2 * jt + n] = keep
            sbuf[2 * jt + n] = give

    def give(jt):
        return pltpu.make_async_remote_copy(
            src_ref=sbuf.at[pl.ds(2 * jt, 2)], dst_ref=out_ref.at[pl.ds(h * 16 + 2 * jt, 2)],
            send_sem=osend.at[jt], recv_sem=orecv.at[jt], device_id=mate, device_id_type=MESH)

    def put(jt):
        return pltpu.make_async_copy(
            obuf.at[pl.ds(2 * jt, 2)], out_ref.at[pl.ds(h * 16 + 2 * jt, 2)], fsem.at[jt])

    def happen(p):
        for name in TIMETABLE.get(p, ()):
            happenings[name]()

    happen(0)
    lax.fori_loop(0, 33, mark, 0)
    load_q.wait()
    r = lax.broadcasted_iota(jnp.int32, (256, 256), 0)
    c = lax.broadcasted_iota(jnp.int32, (256, 256), 1)
    order = jnp.where(c == lax.rem(r, 16) * 16 + r // 16, 1.0, 0.0).astype(BF16)

    def by_head(n, _):
        rows = q_raw[pl.ds(pl.multiple_of(n * 256, 256), 256), :]
        rows = jnp.dot(order, rows, preferred_element_type=F32).astype(BF16)
        for head in range(16):
            q_rows[head, pl.ds(pl.multiple_of(n * 16, 16), 16), :] = rows[head * 16:(head + 1) * 16]
        return 0

    def turn(n, _):
        q_ref[2 * n] = q_rows[2 * n].T
        q_ref[2 * n + 1] = q_rows[2 * n + 1].T
        return 0

    lax.fori_loop(0, 16, by_head, 0, unroll=8)
    lax.fori_loop(0, 8, turn, 0, unroll=4)
    happen(1)
    own_block(0)
    happen(2)
    own_block(1)
    happen(3)
    handed(*SLABS[0])
    places = [chips(*s) for s in SLABS]

    def out_of(jt):
        give(jt).start()
        put(jt).start()

    m = step(None, None, None, places[0], SLABS[0][0] * 4)
    for n in range(6):
        g, cur = SLABS[n][0], places[n]

        def one(j, m, n=n, g=g, cur=cur):
            for at in range(4):
                if 4 + 4 * n + at in TIMETABLE:
                    pl.when(j == at)(lambda at=at: happen(4 + 4 * n + at))
            pl.when(j == 3)(lambda: handed(*SLABS[n + 1]))
            jt = g * 4 + j
            nxt = [(jnp.where(j < 3, a, c), jnp.where(j < 3, b, d)) for (a, b), (c, d) in zip(cur, places[n + 1])]
            m = step(cur, jt, m, nxt, jnp.where(j < 3, jt + 1, SLABS[n + 1][0] * 4))
            if n == 4:
                pl.when(j > 0)(lambda: out_of(jt - 1))
                finish(jt)
            return m

        m = lax.fori_loop(0, 4, one, m)
        if n == 4:
            out_of(3)

    def two(j, m):
        @pl.when(j == 0)
        def _():
            happen(28)
            handed(*SLABS[7])
        jt = 4 + j
        m = step(places[6], jt, m, places[7], jt)
        pl.when(j > 0)(lambda: out_of(jt - 1))
        m = step(places[7], jt, m, places[6], jt + 1)
        finish(jt)
        return m

    m = lax.fori_loop(0, 3, two, m)
    m = step(places[6], 7, m, places[7], 7)
    out_of(6)
    step(places[7], 7, m, None, None)
    finish(7)
    out_of(7)
    ending[0] = True
    first()
    for p in TIMETABLE:
        happen(p)
    for jt in range(8):
        give(jt).wait_send()
        put(jt).wait()
    for jt in range(8):
        give(jt).wait_recv()


N_SENDS = 128


def body(queries, key_rows, value_vectors, doc_ids):
    tokens, heads, size = queries.shape
    groups = key_rows.shape[1]
    q = queries.reshape(tokens * heads, size)
    kk = key_rows.transpose(1, 0, 2)
    vv = value_vectors.reshape(2, 128, groups, size).transpose(2, 0, 3, 1).reshape(groups, 256, 128)
    scale = LOG2E * size ** -0.5
    vmem, anyspace = pl.BlockSpec(memory_space=pltpu.VMEM), pl.BlockSpec(memory_space=pl.ANY)
    out = pl.pallas_call(
        functools.partial(kernel, scale),
        out_shape=jax.ShapeDtypeStruct((2 * heads, 128, size), BF16),
        in_specs=[anyspace, anyspace, anyspace, vmem],
        out_specs=anyspace,
        scratch_shapes=[
            pltpu.VMEM((tokens * heads, size), BF16),
            pltpu.VMEM((heads, tokens, size), BF16),
            pltpu.VMEM((heads, size, tokens), BF16),
            pltpu.VMEM((UNITS, 512, 128), BF16),
            pltpu.VMEM((33, 256, 128), BF16),
            pltpu.VMEM((128, 256), BF16),
            pltpu.VMEM((U, T), F32),
            pltpu.VMEM((8, 128, T), F32),
            pltpu.VMEM((8, 1, T), F32),
            pltpu.VMEM((8, 8, T), F32),
            pltpu.VMEM((heads, 128, size), BF16),
            pltpu.VMEM((heads, 128, size), BF16),
            pltpu.SemaphoreType.DMA((14,)),
            pltpu.SemaphoreType.DMA,
            pltpu.SemaphoreType.DMA((2,)),
            pltpu.SemaphoreType.DMA((N_SENDS,)),
            pltpu.SemaphoreType.DMA((UNITS,)),
            pltpu.SemaphoreType.DMA((8,)),
            pltpu.SemaphoreType.DMA((8,)),
            pltpu.SemaphoreType.DMA((8,)),
        ],
        compiler_params=pltpu.CompilerParams(
            collective_id=0, has_side_effects=True, vmem_limit_bytes=60 * 1024 * 1024),
    )(q, kk, vv, doc_ids.reshape(128, 128))
    return out.transpose(1, 0, 2)


def solution(mesh):
    placed = (P("ctx", "head", None), P("ctx", "head", None), P("ctx", "head", None), P())
    return jax.shard_map(
        body, mesh=mesh, in_specs=placed, out_specs=P(("ctx", "head"), None, None), check_vma=False
    )
```

```python
import functools

import jax
import jax.numpy as jnp
from jax import lax
from jax.experimental import pallas as pl
from jax.experimental.pallas import tpu as pltpu
from jax.sharding import PartitionSpec as P

F32, BF16 = jnp.float32, jnp.bfloat16
MESH = pl.DeviceIdType.MESH
LOG2E = 1.4426950408889634
FAR = -1e30
T = 512
U = 2048
KB = 256
OWN0 = 72
UNITS = 73
NEAR = ((0, 3), (0, 1), (3, 0), (1, 0))
SECOND = ((0, 0), (2, 0), (0, 2), (1, 1))
THIRD = ((1, 3), (3, 1), (3, 3), (2, 1))
LAST = ((2, 3), (1, 2), (3, 2), (2, 2))
TIMETABLE = {
    1: ("e1", "f1", "f1b"),
    2: ("p0",),
    3: ("e2", "e2b", "a0", "a0b"),
    4: ("row2", "p1", "b0", "p3"),
    5: ("b0b",),
    6: ("col2",),
    8: ("a1", "a3b", "a02", "a1b"),
    9: ("b3",),
    10: ("a2", "a3"),
    11: ("p2",),
    13: ("a12", "b1", "a2b"),
    15: ("b1b",),
    16: ("a32", "b2", "a22"),
    18: ("b2b", "b3b"),
    20: ("b23",),
    21: ("b20",),
    22: ("b21",),
    25: ("b22",),
}
SLABS = ((0, NEAR), (1, NEAR), (0, SECOND), (0, THIRD), (0, LAST), (1, SECOND), (1, THIRD), (1, LAST))


def kernel(scale, q_hbm, k_hbm, v_hbm, doc_ref, out_ref, q_raw, q_rows, q_ref, buf, aug, qaug, s_ref, acc, mm, ll, obuf, sbuf,
           lsem, qsem, ysem, ssem, rsem, osend, orecv, fsem):
    i = lax.axis_index("ctx")
    h = lax.axis_index("head")
    k = lax.rem(i, 2)
    z = lax.rem(i // 2, 4)
    x = lax.rem(i // 8, 4)
    y = i // 32
    o = 1 - k
    up = lambda a: lax.rem(a + 1, 4)
    dn = lambda a: lax.rem(a + 3, 4)
    op = lambda a: lax.rem(a + 2, 4)

    def dev(yy, xx, zz, kk, hh=None):
        return {"ctx": ((yy * 4 + xx) * 4 + zz) * 2 + kk, "head": h if hh is None else hh}

    A = lambda zz, xx, kk: (zz * 4 + xx) * 2 + kk
    B = lambda xx, zz, kk: 32 + (xx * 4 + zz) * 2 + kk
    R = lambda zz, kk: 64 + zz * 2 + kk
    right_x, left_x = dev(y, up(x), z, k), dev(y, dn(x), z, k)
    right_z, left_z = dev(y, x, up(z), k), dev(y, x, dn(z), k)
    across, other = dev(1 - y, x, z, k), dev(y, x, z, o)
    mate = dev(y, x, z, k, 1 - h)

    sends = {}
    ending = [False]

    def copy(n, src, dst, to, half=None, sem=None):
        part = () if half is None else (pl.ds(256 * half, 256),)
        return pltpu.make_async_remote_copy(
            src_ref=buf.at[(src,) + part], dst_ref=buf.at[(dst,) + part], send_sem=ssem.at[n],
            recv_sem=rsem.at[dst] if sem is None else sem, device_id=to, device_id_type=MESH)

    def when(cond, f):
        if cond is None:
            f()
        else:
            pl.when(cond)(f)

    def send(name, src, dst, to, cond=None, half=None, sem=None):
        n = sends.setdefault(name, len(sends))

        def go():
            c = copy(n, src, dst, to, half, sem)
            c.wait_send() if ending[0] else c.start()

        when(cond, go)

    def arrived(u, cond=None):
        if not ending[0]:
            when(cond, lambda: copy(0, u, u, other).wait_recv())

    own = jnp.int32(OWN0)
    a_own, b_own = A(z, x, k), B(x, z, k)
    local = [(0, own, None), (1, b_own, None), (0, a_own, y == 0)] + [(1, R(n, k), y == 0) for n in range(4)]

    class local_copy:
        def __init__(self, n):
            g, u, _ = local[n]
            self.both = [
                pltpu.make_async_copy(k_hbm.at[g], buf.at[u, 0:256], lsem.at[2 * n]),
                pltpu.make_async_copy(v_hbm.at[g], buf.at[u, 256:512], lsem.at[2 * n + 1])]

        def start(self):
            for c in self.both:
                c.start()

        def wait(self):
            for c in self.both:
                c.wait()

    for n in range(len(local)):
        when(local[n][2], lambda n=n: local_copy(n).start())
    load_q = pltpu.make_async_copy(q_hbm, q_raw, qsem)
    load_q.start()
    barrier = pltpu.get_barrier_semaphore()
    for to in (right_x, left_x, right_z, left_z, across, other, mate):
        pl.semaphore_signal(barrier, inc=1, device_id=to, device_id_type=MESH)
    pl.semaphore_wait(barrier, 7)
    for n in range(len(local)):
        when(local[n][2], lambda n=n: local_copy(n).wait())

    def relay(name, even, place, at, to_r, to_l):
        src = jnp.where(even, place(dn(at)), place(up(at)))
        send(name + "r", src, src, to_r, even)
        send(name + "l", src, src, to_l, jnp.logical_not(even))

    def over(name, u, cond=None):
        send("o" + name, u, u, other, cond)

    x_even, z_even = lax.rem(x, 2) == 0, lax.rem(z, 2) == 0
    sign = {0: z_even, 1: jnp.logical_not(z_even), 2: z_even, 3: jnp.logical_not(z_even)}

    def row_on(name, zz):
        u = B(x, zz, k)
        send(name + "y", u, R(zz, k), across, y == 0)
        send(name + "r", u, u, right_x, x < 3)
        send(name + "l", u, u, left_x, x == 0)

    def before_on(n, zz):
        arrived(R(zz, k), y == 1)
        u = B(x, zz, k)
        send(f"pr{n}", R(zz, k), u, right_x, x == 3)
        send(f"pl{n}", R(zz, k), u, left_x, x > 0)
        if n == 0:
            over("p0", R(z, 1), k == 1)
        else:
            over(f"p{n}", R(zz, k), zz > z)

    zs = {0: z, 1: up(z), 2: op(z), 3: dn(z)}
    xs = {0: x, 1: up(x), 2: op(x), 3: dn(x)}

    def nearer(even, at, first):
        return jnp.where(even == first, dn(at), up(at))

    def row_here(name, zz, first=False):
        arrived(B(x, zz, k))
        if first:
            relay("bz", z_even, lambda c: B(x, c, k), z, right_z, left_z)
        row_on(name, zz)
        over(name, B(x, zz, k), zz < z)

    def col_here(name, xx, first=False):
        u = A(z, xx, k)
        arrived(u)
        if first:
            relay("ax", x_even, lambda c: A(z, c, k), x, right_x, left_x)
        send(name + "zr", u, u, right_z)
        send(name + "zl", u, u, left_z)
        over(name, u)

    def a_here(n, zz, first=False):
        u = A(zz, xs[n], k)
        arrived(u)
        if first:
            relay(f"az{n}", sign[n], lambda c: A(c, xs[n], k), z, right_z, left_z)
        over(f"a{n}{'n' if first else 'f'}", u)

    def a_opposite(n):
        u = A(zs[2], xs[n], k)
        arrived(u)
        over(f"a{n}2", u)

    def b_here(n, xx, first=False):
        u = B(xx, zs[n], k)
        arrived(u)
        if first:
            relay(f"bx{n}", x_even, lambda c: B(c, zs[n], k), x, right_x, left_x)
        over(f"b{n}{'n' if first else 'f'}", u)

    def b_opposite(n):
        u = B(xs[2], zs[n], k)
        arrived(u)
        over(f"b2{n}", u)

    def previous():
        for half in range(2):
            if not ending[0]:
                when(y == 1, lambda: copy(0, a_own, a_own, other, half, ysem.at[half]).wait_recv())
            send(f"pxr{half}", a_own, a_own, right_x, x == 3, half)
            send(f"pxl{half}", a_own, a_own, left_x, x > 0, half)
            send(f"pzr{half}", a_own, a_own, right_z, z == 3, half)
            send(f"pzl{half}", a_own, a_own, left_z, z > 0, half)
        over("a00", A(z, x, 1), k == 1)

    happenings = {
        "e1": previous,
        "f1": lambda: row_here("f1", nearer(z_even, z, True), True),
        "f1b": lambda: row_here("f1b", nearer(z_even, z, False)),
        "row2": lambda: row_here("row2", zs[2]),
        "e2": lambda: col_here("e2", nearer(x_even, x, True), True),
        "e2b": lambda: col_here("e2b", nearer(x_even, x, False)),
        "col2": lambda: col_here("col2", xs[2]),
    }
    for n in range(4):
        happenings[f"p{n}"] = lambda n=n: before_on(n, zs[n])
        happenings[f"a{n}"] = lambda n=n: a_here(n, nearer(sign[n], z, True), True)
        happenings[f"a{n}b"] = lambda n=n: a_here(n, nearer(sign[n], z, False))
        happenings[f"a{n}2"] = lambda n=n: a_opposite(n)
        happenings[f"b{n}"] = lambda n=n: b_here(n, nearer(x_even, x, True), True)
        happenings[f"b{n}b"] = lambda n=n: b_here(n, nearer(x_even, x, False))
        happenings[f"b2{n}"] = lambda n=n: b_opposite(n)

    def handed(g, slab):
        for dx, dz in slab:
            xx, zz = xs[dx], zs[dz]
            if g == 0:
                arrived(A(zz, xx, o))
            elif dx:
                arrived(B(xx, zz, o))
            elif dz:
                arrived(jnp.where(zz < z, B(x, zz, o), R(zz, o)))
            else:
                arrived(jnp.where(k == 0, R(z, o), B(x, z, o)))

    def first():
        send("y0", own, a_own, across, y == 0, 0, ysem.at[0])
        send("y1", own, a_own, across, y == 0, 1, ysem.at[1])
        send("bzr", b_own, b_own, right_z)
        send("bzl", b_own, b_own, left_z)
        send("xr", own, a_own, right_x, x < 3)
        send("xl", own, a_own, left_x, x == 0)
        send("zr", own, a_own, right_z, z < 3)
        send("zl", own, a_own, left_z, z == 0)
        row_on("own", z)
        send("own0", own, A(z, x, 0), other, k == 0)
        send("own1", b_own, B(x, z, 0), other, k == 0)

    first()

    docs = doc_ref[...]
    first1 = jnp.sum((docs < 1).astype(F32), keepdims=True).astype(jnp.int32)
    first2 = jnp.sum((docs < 2).astype(F32), keepdims=True).astype(jnp.int32)
    lane = lax.broadcasted_iota(jnp.int32, (1, 128), 1)
    none = jnp.int32(1 << 30)
    lo = jnp.where(lane == 0, 0, jnp.where(lane == 1, first1, jnp.where(lane == 2, first2, jnp.where(lane == 3, -none, none))))
    hi = jnp.where(lane == 0, first1, jnp.where(lane == 1, first2, jnp.where(lane == 2, none, jnp.where(lane == 3, 0, -none))))
    p = x * 4 + z
    me = i * 256

    def mark(u, _):
        c, kk = u // 2, lax.rem(u, 2)
        yy = jnp.where(c < p, y, y - 1)
        base = ((yy * 16 + c) * 2 + kk) * 256
        inner = jnp.where(kk == k, -100000, jnp.where(k == 0, ((y * 16 - 16 + c) * 2 + 1) * 256, (y * 16 + c) * 512))
        base = jnp.where(u == 32, me, jnp.where(c == p, inner, base))
        row = base + lax.broadcasted_iota(jnp.int32, (256, 128), 0)
        aug[u] = jnp.where((row >= lo) & (row < hi), 1.0, 0.0).astype(BF16)
        return 0

    pos = me + lax.broadcasted_iota(jnp.int32, (128, 256), 1)
    mine = (pos >= first1).astype(jnp.int32) + (pos >= first2).astype(jnp.int32)
    d = lax.broadcasted_iota(jnp.int32, (128, 256), 0)
    qaug[...] = jnp.where((d < 4) & ((d == 3) | (mine != d)), FAR, 0.0).astype(BF16)

    def query(jt):
        top = jnp.concatenate([q_ref[2 * jt], q_ref[2 * jt + 1]], axis=1)
        low = jnp.concatenate([qaug[...], qaug[...]], axis=1)
        return jnp.concatenate([top, low], axis=0)

    def keys(u, au):
        return jnp.concatenate([buf[u, 0:256, :], aug[au]], axis=1)

    def values(u):
        return jnp.concatenate([buf[u, 256:384, :], buf[u, 384:512, :]], axis=1)

    def eighths(a, f):
        return f(a.reshape(a.shape[0] // 8, 8, T), axis=0)

    def own_block(g):
        u = own if g == 0 else b_own

        def tile(j, _):
            jt = g * 4 + j
            s = jnp.dot(keys(u, 32), query(jt), preferred_element_type=F32)
            key = lax.broadcasted_iota(jnp.int32, (256, T), 0)
            tok = lax.rem(lax.broadcasted_iota(jnp.int32, (256, T), 1), 256)
            s = jnp.where(key <= tok, s, FAR)
            m = jnp.max(s, axis=0, keepdims=True)
            w = jnp.exp2((s - m) * scale)
            mm[jt] = m
            ll[jt] = eighths(w, jnp.sum)
            acc[jt] = jnp.dot(values(u), w.astype(BF16), preferred_element_type=F32)
            return 0

        lax.fori_loop(0, 4, tile, 0, unroll=2)

    def chips(g, slab):
        found = []
        for dx, dz in slab:
            xx, zz = xs[dx], zs[dz]
            if g == 0:
                c = zz * 4 + xx
            elif dx:
                c = 16 + xx * 4 + zz
            elif dz:
                c = jnp.where(zz < z, 16 + x * 4 + zz, 32 + zz)
            else:
                c = jnp.where(k == 0, 32 + z, 16 + x * 4 + z)
            found.append((c * 2, (xx * 4 + zz) * 2))
        return found

    def step(cur, jt, m_cur, nxt, jn):
        if nxt is not None:
            q = query(jn)
        if cur is not None:
            m_old = mm[jt]
            m_new = jnp.maximum(m_old, m_cur)
            alpha = jnp.exp2((m_old - m_new) * scale)
            mm[jt] = m_new
            out = acc[jt] * alpha
            total = ll[jt] * alpha
        best = None
        for b in range(U // KB):
            rows = slice(b * KB, (b + 1) * KB)
            if cur is not None:
                w = jnp.exp2((s_ref[rows] - m_new) * scale)
                total = total + eighths(w, jnp.sum)
                w = w.astype(BF16)
            if nxt is not None:
                u, au = nxt[b // 2]
                s = jnp.dot(keys(u + b % 2, au + b % 2), q, preferred_element_type=F32)
                high = eighths(s, jnp.max)
                best = high if best is None else jnp.maximum(best, high)
                s_ref[rows] = s
            if cur is not None:
                out = out + jnp.dot(values(cur[b // 2][0] + b % 2), w, preferred_element_type=F32)
        if cur is not None:
            acc[jt] = out
            ll[jt] = total
        return None if nxt is None else jnp.max(best, axis=0, keepdims=True)

    def finish(jt):
        total = jnp.sum(ll[jt], axis=0, keepdims=True)
        done = acc[jt] / total
        for n in range(2):
            head = done[:, n * 256:(n + 1) * 256].T.astype(BF16)
            keep = jnp.where(h == 0, head[:128], head[128:])
            give = jnp.where(h == 0, head[128:], head[:128])
            obuf[2 * jt + n] = keep
            sbuf[2 * jt + n] = give

    def give(jt):
        return pltpu.make_async_remote_copy(
            src_ref=sbuf.at[pl.ds(2 * jt, 2)], dst_ref=out_ref.at[pl.ds(h * 16 + 2 * jt, 2)],
            send_sem=osend.at[jt], recv_sem=orecv.at[jt], device_id=mate, device_id_type=MESH)

    def put(jt):
        return pltpu.make_async_copy(
            obuf.at[pl.ds(2 * jt, 2)], out_ref.at[pl.ds(h * 16 + 2 * jt, 2)], fsem.at[jt])

    def happen(p):
        for name in TIMETABLE.get(p, ()):
            happenings[name]()

    happen(0)
    lax.fori_loop(0, 33, mark, 0, unroll=3)
    load_q.wait()
    r = lax.broadcasted_iota(jnp.int32, (256, 256), 0)
    c = lax.broadcasted_iota(jnp.int32, (256, 256), 1)
    order = jnp.where(c == lax.rem(r, 16) * 16 + r // 16, 1.0, 0.0).astype(BF16)

    def by_head(n, _):
        rows = q_raw[pl.ds(pl.multiple_of(n * 256, 256), 256), :]
        rows = jnp.dot(order, rows, preferred_element_type=F32).astype(BF16)
        for head in range(16):
            q_rows[head, pl.ds(pl.multiple_of(n * 16, 16), 16), :] = rows[head * 16:(head + 1) * 16]
        return 0

    def turn(n, _):
        q_ref[2 * n] = q_rows[2 * n].T
        q_ref[2 * n + 1] = q_rows[2 * n + 1].T
        return 0

    lax.fori_loop(0, 16, by_head, 0, unroll=8)
    lax.fori_loop(0, 8, turn, 0, unroll=4)
    happen(1)
    own_block(0)
    happen(2)
    own_block(1)
    happen(3)
    handed(*SLABS[0])
    places = [chips(*s) for s in SLABS]

    def out_of(jt):
        give(jt).start()
        put(jt).start()

    m = step(None, None, None, places[0], SLABS[0][0] * 4)
    for n in range(6):
        g, cur = SLABS[n][0], places[n]

        def one(j, m, n=n, g=g, cur=cur):
            for at in range(4):
                if 4 + 4 * n + at in TIMETABLE:
                    pl.when(j == at)(lambda at=at: happen(4 + 4 * n + at))
            pl.when(j == 3)(lambda: handed(*SLABS[n + 1]))
            jt = g * 4 + j
            nxt = [(jnp.where(j < 3, a, c), jnp.where(j < 3, b, d)) for (a, b), (c, d) in zip(cur, places[n + 1])]
            m = step(cur, jt, m, nxt, jnp.where(j < 3, jt + 1, SLABS[n + 1][0] * 4))
            if n == 4:
                pl.when(j > 0)(lambda: out_of(jt - 1))
                finish(jt)
            return m

        m = lax.fori_loop(0, 4, one, m)
        if n == 4:
            out_of(3)

    def two(j, m):
        @pl.when(j == 0)
        def _():
            happen(28)
            handed(*SLABS[7])
        jt = 4 + j
        m = step(places[6], jt, m, places[7], jt)
        pl.when(j > 0)(lambda: out_of(jt - 1))
        m = step(places[7], jt, m, places[6], jt + 1)
        finish(jt)
        return m

    m = lax.fori_loop(0, 3, two, m)
    m = step(places[6], 7, m, places[7], 7)
    out_of(6)
    step(places[7], 7, m, None, None)
    finish(7)
    out_of(7)
    ending[0] = True
    first()
    for p in TIMETABLE:
        happen(p)
    for jt in range(8):
        give(jt).wait_send()
        put(jt).wait()
    for jt in range(8):
        give(jt).wait_recv()


N_SENDS = 128


def body(queries, key_rows, value_vectors, doc_ids):
    tokens, heads, size = queries.shape
    groups = key_rows.shape[1]
    q = queries.reshape(tokens * heads, size)
    kk = key_rows.transpose(1, 0, 2)
    vv = value_vectors.reshape(2, 128, groups, size).transpose(2, 0, 3, 1).reshape(groups, 256, 128)
    scale = LOG2E * size ** -0.5
    vmem, anyspace = pl.BlockSpec(memory_space=pltpu.VMEM), pl.BlockSpec(memory_space=pl.ANY)
    out = pl.pallas_call(
        functools.partial(kernel, scale),
        out_shape=jax.ShapeDtypeStruct((2 * heads, 128, size), BF16),
        in_specs=[anyspace, anyspace, anyspace, vmem],
        out_specs=anyspace,
        scratch_shapes=[
            pltpu.VMEM((tokens * heads, size), BF16),
            pltpu.VMEM((heads, tokens, size), BF16),
            pltpu.VMEM((heads, size, tokens), BF16),
            pltpu.VMEM((UNITS, 512, 128), BF16),
            pltpu.VMEM((33, 256, 128), BF16),
            pltpu.VMEM((128, 256), BF16),
            pltpu.VMEM((U, T), F32),
            pltpu.VMEM((8, 128, T), F32),
            pltpu.VMEM((8, 1, T), F32),
            pltpu.VMEM((8, 8, T), F32),
            pltpu.VMEM((heads, 128, size), BF16),
            pltpu.VMEM((heads, 128, size), BF16),
            pltpu.SemaphoreType.DMA((14,)),
            pltpu.SemaphoreType.DMA,
            pltpu.SemaphoreType.DMA((2,)),
            pltpu.SemaphoreType.DMA((N_SENDS,)),
            pltpu.SemaphoreType.DMA((UNITS,)),
            pltpu.SemaphoreType.DMA((8,)),
            pltpu.SemaphoreType.DMA((8,)),
            pltpu.SemaphoreType.DMA((8,)),
        ],
        compiler_params=pltpu.CompilerParams(
            collective_id=0, has_side_effects=True, vmem_limit_bytes=60 * 1024 * 1024),
    )(q, kk, vv, doc_ids.reshape(128, 128))
    return out.transpose(1, 0, 2)


def solution(mesh):
    placed = (P("ctx", "head", None), P("ctx", "head", None), P("ctx", "head", None), P())
    return jax.shard_map(
        body, mesh=mesh, in_specs=placed, out_specs=P(("ctx", "head"), None, None), check_vma=False
    )
```
